32 devices in a mesh: rows: 16 (over z, y, x), cent: 2 (over core).
Axes of the slice: x: 2, y: 2, z: 4, core: 2. Of those that a mesh axis runs over, the one named last changes fastest.
Arguments:
- points: bfloat16 [16384, 1024], P('rows'), may hold values from -8 to 8
- centroids: bfloat16 [4096, 1024], P('cent'), may hold values from -8 to 8
- assign: int32 [16384], P('rows'), may hold values from 0 to 4095, as said below
Outputs:
- nearest: float32 [2, 16384], P(None, 'rows')
- updated: bfloat16 [4096, 1024], P('cent')
The draws below stay inside these ranges and needn't reach their ends.
Inputs may be any that keep to these rules, and one draw needn't show every extreme that they name: `assign`: split the points into aligned blocks of 1024 and the centroids into aligned groups of 128 consecutive ones: in each block at most 64 points are assigned into any one group, and in every block some group takes exactly 64 of them.
All inputs are finite; a program needn't handle non-finite values.
Results may differ from the reference program's by a relative error of at most 0.001.
Values may be sent and summed in bfloat16 or wider, within the bound.
A program may use at most 64 MiB of HBM per device.

```python
import jax
import jax.numpy as jnp
from jax import lax

D = 1024
K = 4096
PTS_DEV = 1024
P_SIZE = 16384
GROUPS = 32
SHARE = 128
CAP = 64


def centroid_field(key):
    key_dir, key_len = jax.random.split(jax.random.fold_in(key, 23), 2)
    raw = jax.random.normal(key_dir, (K, D), jnp.float32)
    length = jax.random.uniform(key_len, (K, 1), jnp.float32, 0.97, 1.03)
    return raw * (length * jnp.sqrt(jnp.float32(D)) / jnp.sqrt(jnp.sum(raw * raw, axis=1, keepdims=True)))


def draw_centroids(key, part):
    return centroid_field(key).astype(jnp.bfloat16)


def draw_points(key, part):
    key_val, key_scale, key_pick = jax.random.split(jax.random.fold_in(key, 37), 3)
    cents = centroid_field(key).astype(jnp.bfloat16).astype(jnp.float32)
    picks = jax.random.randint(key_pick, (P_SIZE,), 0, K)
    noise = jax.random.normal(key_val, (P_SIZE, D), jnp.float32)
    low, high = (0.2, 1.5)
    logs = jax.random.uniform(key_scale, (P_SIZE, 1), jnp.float32, jnp.log(low), jnp.log(high))
    scaled = jnp.clip(jnp.exp(logs) * cents[picks] + 0.3 * noise, -8.0, 8.0)
    return scaled.astype(jnp.bfloat16)


def draw_assign(key, part):
    blocks_total = P_SIZE // PTS_DEV
    key_block, key_order, key_shuffle, key_offset = jax.random.split(jax.random.fold_in(key, 11), 4)
    picked = jax.random.randint(key_block, (blocks_total,), 0, GROUPS)
    slot_group = jnp.repeat(jnp.arange(GROUPS, dtype=jnp.int32), CAP)

    def one_block(index):
        order = jax.random.permutation(jax.random.fold_in(key_order, index), GROUPS * CAP).astype(jnp.int32)
        forced = slot_group == picked[index]
        score = jnp.where(forced, order - GROUPS * CAP, order)
        chosen = slot_group[jnp.argsort(score, stable=True)[:PTS_DEV]]
        mixing = jax.random.permutation(jax.random.fold_in(key_shuffle, index), PTS_DEV)
        return chosen[mixing]
    groups_all = jax.vmap(one_block)(jnp.arange(blocks_total, dtype=jnp.int32))
    offsets = jax.random.randint(key_offset, (blocks_total, PTS_DEV), 0, SHARE)
    return (groups_all * SHARE + offsets).reshape(P_SIZE).astype(jnp.int32)


def setup_inputs(seed: int = 0) -> dict:
    arg_keys = jax.random.split(jax.random.key(seed), 4)
    return {
        "points": draw_points(jax.random.fold_in(arg_keys[3], 71), 0),
        "centroids": draw_centroids(jax.random.fold_in(arg_keys[3], 71), 0),
        "assign": draw_assign(jax.random.fold_in(arg_keys[3], 71), 0),
    }


def smallest(points, pnorm, cents):
    cnorm = jnp.sum(jnp.square(cents.astype(jnp.float32)), axis=1)
    size = P_SIZE
    if P_SIZE % 1024 == 0:
        size = 1024

    def one_block(pair):
        block, norms = pair
        dots = lax.dot_general(block, cents, (((1,), (1,)), ((), ())), preferred_element_type=jnp.float32)
        return jnp.min((norms[:, None] - 2.0 * dots + cnorm[None, :]) / D, axis=1)

    result = lax.map(one_block, (points.reshape(P_SIZE // size, size, D), pnorm.reshape(P_SIZE // size, size)))
    return result.reshape(P_SIZE)


def reference(points, centroids, assign):
    wide = points.astype(jnp.float32)
    pnorm = jnp.sum(jnp.square(wide), axis=1)
    first = smallest(points, pnorm, centroids)
    sums = jax.ops.segment_sum(wide, assign, num_segments=K)
    counts = jax.ops.segment_sum(jnp.ones((P_SIZE,), jnp.float32), assign, num_segments=K)
    updated = ((sums + centroids.astype(jnp.float32)) / (counts[:, None] + 1.0)).astype(jnp.bfloat16)
    second = smallest(points, pnorm, updated)
    return jnp.stack([first, second]), updated
```

```python
import functools

import jax
import jax.numpy as jnp
from jax import lax
from jax.experimental import pallas as pl
from jax.experimental.pallas import tpu as pltpu
from jax.sharding import PartitionSpec as P


def smallest(points, pnorm, cents):
    cnorm = jnp.sum(jnp.square(cents.astype(jnp.float32)), axis=1)
    dots = lax.dot_general(
        points, cents, (((1,), (1,)), ((), ())), preferred_element_type=jnp.float32
    )
    return jnp.min((pnorm[:, None] - 2.0 * dots + cnorm[None, :]) / points.shape[1], axis=1)


def block_min(values):
    return lax.pmin(values, "cent")


def renew(part_sums, part_counts, own_rows):
    return ((part_sums + own_rows.astype(jnp.float32)) / (part_counts[:, None] + 1.0)).astype(
        jnp.bfloat16
    )


def per_device(points, centroids, assign):
    blocksize = centroids.shape[0]
    count_pts = points.shape[0]
    pnorm = jnp.sum(jnp.square(points.astype(jnp.float32)), axis=1)
    first = smallest(points, pnorm, centroids)
    first = block_min(first)
    relative = assign - lax.axis_index("cent") * blocksize
    share = blocksize // lax.axis_size("rows")
    own = lax.dynamic_slice_in_dim(centroids, lax.axis_index("rows") * share, share, 0)
    rows_count = lax.axis_size("rows")
    groups = rows_count * lax.axis_size("cent")
    capacity = max(2, 2 * count_pts // groups)
    inside = (relative >= 0) & (relative < blocksize)
    owners = jnp.where(inside, relative // share, rows_count)
    offsets = jnp.where(inside, relative - relative // share * share, 0)
    owner_hot = owners[:, None] == lax.broadcasted_iota(jnp.int32, (count_pts, rows_count), 1)
    earlier = lax.broadcasted_iota(jnp.int32, (count_pts, count_pts), 1) < lax.broadcasted_iota(
        jnp.int32, (count_pts, count_pts), 0
    )
    before = jnp.dot(
        earlier.astype(jnp.bfloat16),
        owner_hot.astype(jnp.bfloat16),
        preferred_element_type=jnp.float32,
    )
    ranking = jnp.sum(jnp.where(owner_hot, before, 0.0), axis=1).astype(jnp.int32)
    slot_index = jnp.where(inside, owners * capacity + ranking, -1)
    placing = (
        lax.broadcasted_iota(jnp.int32, (rows_count * capacity, count_pts), 0)
        == slot_index[None, :]
    )
    outgoing = jnp.dot(
        placing.astype(jnp.bfloat16), points, preferred_element_type=jnp.float32
    ).astype(jnp.bfloat16)
    labels = (jnp.sum(jnp.where(placing, offsets[None, :] + 1, 0), axis=1) - 1).astype(jnp.bfloat16)
    arrived, arrived_labels = (
        lax.all_to_all(outgoing, "rows", split_axis=0, concat_axis=0, tiled=True),
        lax.all_to_all(labels, "rows", split_axis=0, concat_axis=0, tiled=True),
    )
    chosen = (
        lax.broadcasted_iota(jnp.int32, (share, arrived.shape[0]), 0)
        == arrived_labels.astype(jnp.int32)[None, :]
    )
    part_sums = jnp.dot(chosen.astype(jnp.bfloat16), arrived, preferred_element_type=jnp.float32)
    part_counts = jnp.sum(chosen.astype(jnp.float32), axis=1)
    updated = lax.all_gather(renew(part_sums, part_counts, own), "rows", axis=0, tiled=True)
    second = smallest(points, pnorm, updated)
    nearest = jnp.stack([first, block_min(second)])
    return (nearest, updated)


PLANE = 4
LANES = 128
VMEM_BYTES = 60 * 1024 * 1024


def nt_dot(a, b):
    return lax.dot_general(a, b, (((1,), (1,)), ((), ())), preferred_element_type=jnp.float32)


def column_min(cents, points):
    wide = cents.astype(jnp.float32)
    cnorm = jnp.sum(wide * wide, axis=1, keepdims=True)
    return jnp.min(cnorm - 2.0 * nt_dot(cents, points), axis=0, keepdims=True)


def lloyd_kernel(
    rows, cap, share, assign_ref, pnorm_ref, points_ref, cents_ref, near_ref, upd_ref,
    send, lab_send, arrived, lab_arrived, acc, gath, mine, theirs, low,
    sent_pts, got_pts, sent_lab, got_lab, own_sem,
    sent_z, sent_x, sent_y, got_full, sent_dx, sent_dy, got_dx, got_dy, out_sem, sent_min, got_min,
):
    count_pts, width = points_ref.shape
    blocksize = cents_ref.shape[0]
    planes = rows // PLANE
    per = LANES // cap
    me = lax.axis_index("rows")
    core = lax.axis_index("cent")
    z, q = me // PLANE, me % PLANE
    xpeer = me + 1 - 2 * (q % 2)
    ypeer = me + 2 - 4 * (q // 2)
    diag = ypeer + 1 - 2 * (q % 2)
    partner = 1 - core

    barrier = pltpu.get_barrier_semaphore()
    for step in range(1, rows):
        pl.semaphore_signal(barrier, inc=1, device_id={"rows": (me + step) % rows})
    pl.semaphore_signal(barrier, inc=1, device_id={"cent": partner})

    relative = (assign_ref[...] - core * blocksize).astype(jnp.float32)
    inside = (relative >= 0.0) & (relative < float(blocksize))
    owner = jnp.where(inside, jnp.floor(relative * (1.0 / share)), float(rows))
    offset1 = jnp.where(inside, relative - owner * share + 1.0, 0.0)
    hot = lax.broadcasted_iota(jnp.int32, (rows, count_pts), 0).astype(jnp.float32) == owner
    hot_f = jnp.where(hot, 1.0, 0.0)
    seg = 256
    tri = jnp.where(
        lax.broadcasted_iota(jnp.int32, (seg, seg), 0) < lax.broadcasted_iota(jnp.int32, (seg, seg), 1),
        1.0, 0.0,
    ).astype(jnp.bfloat16)
    carry = jnp.zeros((rows, 1), jnp.float32)
    pieces = []
    for s in range(count_pts // seg):
        part = hot_f[:, s * seg:(s + 1) * seg]
        before = jnp.dot(part.astype(jnp.bfloat16), tri, preferred_element_type=jnp.float32) + carry
        pieces.append(jnp.sum(part * before, axis=0, keepdims=True))
        carry = carry + jnp.sum(part, axis=1, keepdims=True)
    ranking = jnp.concatenate(pieces, axis=1)
    slot = jnp.where(inside, owner * cap + ranking, -1.0)
    labels8 = jnp.broadcast_to(offset1, (8, count_pts)).astype(jnp.bfloat16)

    pl.semaphore_wait(barrier, rows)

    order = [planes // 2] + [o for o in range(1, planes) if o != planes // 2] + [0]
    chunk = PLANE * cap
    a2a = []

    def ship(src, dst, ss, rs, axis, target):
        copy = pltpu.make_async_remote_copy(
            src_ref=src, dst_ref=dst, send_sem=ss, recv_sem=rs, device_id={axis: target}
        )
        copy.start()
        return copy

    own_copies = []
    for j, o in enumerate(order):
        zt = (z + o) % planes
        placing = jnp.where(
            (lax.broadcasted_iota(jnp.int32, (chunk, count_pts), 0) + zt * chunk).astype(jnp.float32)
            == slot, 1.0, 0.0,
        ).astype(jnp.bfloat16)
        lab = nt_dot(labels8, placing)
        for t in range(chunk // LANES):
            lab_send[j, t] = lab[:, t * LANES:(t + 1) * LANES]
        send[j] = jnp.dot(
            placing, points_ref[...], preferred_element_type=jnp.float32
        ).astype(jnp.bfloat16)
        for k in range(PLANE):
            i = (q + k) % PLANE
            target = zt * PLANE + i
            piece = send.at[j, pl.ds(pl.multiple_of(i * cap, cap), cap)]
            lab_piece = lab_send.at[j, i // per]
            spot = arrived.at[me]
            if o == 0 and k == 0:
                for n, (a, b) in enumerate(((piece, spot), (lab_piece, lab_arrived.at[me]))):
                    c = pltpu.make_async_copy(a, b, own_sem.at[n])
                    c.start()
                    own_copies.append(c)
            else:
                n = j * PLANE + k
                a2a.append(ship(lab_piece, lab_arrived.at[me], sent_lab.at[n], got_lab.at[me], "rows", target))
                a2a.append(ship(piece, spot, sent_pts.at[n], got_pts.at[me], "rows", target))

    pnorm = pnorm_ref[...]
    kb = 512
    low[...] = jnp.full(low.shape, jnp.inf, jnp.float32)

    def first_step(i, _):
        block = cents_ref[pl.ds(pl.multiple_of(i * kb, kb), kb), :]
        low[0:1, :] = jnp.minimum(low[0:1, :], column_min(block, points_ref[...]))
        return 0

    lax.fori_loop(0, blocksize // kb, first_step, 0)
    mine[0] = (pnorm + low[0:1, :]) / width
    min_copies = [ship(mine.at[0], theirs.at[0], sent_min.at[0], got_min.at[0], "cent", partner)]

    acc[...] = jnp.zeros_like(acc)
    counts = jnp.zeros((share, 1), jnp.float32)
    rowid1 = lax.broadcasted_iota(jnp.int32, (share, cap), 0).astype(jnp.float32) + 1.0
    for c in own_copies:
        c.wait()
    for o in [0] + [o for o in order if o != 0]:
        zs = (z + planes - o) % planes
        total = None
        for k in range(PLANE):
            i = (q + PLANE - k) % PLANE
            source = zs * PLANE + i
            if not (o == 0 and k == 0):
                for ref, sem in ((lab_arrived, got_lab), (arrived, got_pts)):
                    pltpu.make_async_remote_copy(
                        src_ref=ref.at[source], dst_ref=ref.at[source], send_sem=own_sem.at[0],
                        recv_sem=sem.at[source], device_id={"rows": source},
                    ).wait_recv()
            lab = lab_arrived[source]
            pick = lab[0:1, 0:cap]
            for t in range(1, per):
                pick = jnp.where(q % per == t, lab[0:1, t * cap:(t + 1) * cap], pick)
            chosen = jnp.where(rowid1 == pick, 1.0, 0.0)
            counts = counts + jnp.sum(chosen, axis=1, keepdims=True)
            acc[...] += jnp.dot(
                chosen.astype(jnp.bfloat16), arrived[source], preferred_element_type=jnp.float32
            )
    own_rows = cents_ref[pl.ds(pl.multiple_of(me * share, share), share), :]
    gath[me] = ((acc[...] + own_rows.astype(jnp.float32)) / (counts + 1.0)).astype(jnp.bfloat16)

    flying = []
    outs = []
    half = share // 2

    def pass_on(block, n):
        flying.append(ship(gath.at[block], gath.at[block], sent_x.at[n], got_full.at[block], "rows", xpeer))
        flying.append(ship(gath.at[block], gath.at[block], sent_y.at[n], got_full.at[block], "rows", ypeer))

    def await_full(block):
        pltpu.make_async_remote_copy(
            src_ref=gath.at[block], dst_ref=gath.at[block], send_sem=own_sem.at[0],
            recv_sem=got_full.at[block], device_id={"rows": xpeer},
        ).wait_recv()

    def await_part(block, part, sem):
        pltpu.make_async_remote_copy(
            src_ref=gath.at[block, part], dst_ref=gath.at[block, part], send_sem=own_sem.at[0],
            recv_sem=sem.at[block], device_id={"rows": xpeer},
        ).wait_recv()

    low[...] = jnp.full(low.shape, jnp.inf, jnp.float32)

    def absorb(block):
        c = pltpu.make_async_copy(gath.at[block], upd_ref.at[block], out_sem.at[block])
        c.start()
        outs.append(c)
        low[0:1, :] = jnp.minimum(low[0:1, :], column_min(gath[block], points_ref[...]))

    pass_on(me, 0)
    line = [1, planes - 1] + [o for o in range(2, planes - 1)] if planes > 2 else list(range(1, planes))
    for n, o in enumerate(line):
        target = ((z + o) % planes) * PLANE + q
        flying.append(ship(gath.at[me], gath.at[me], sent_z.at[n], got_full.at[me], "rows", target))
    absorb(me)
    upper, lower = pl.ds(0, half), pl.ds(half, half)
    delays = [0] + [planes - o for o in line]
    for n, o in enumerate(delays):
        zs = (z + o) % planes
        if n > 0:
            await_full(zs * PLANE + q)
            pass_on(zs * PLANE + q, n)
        by, bx = zs * PLANE + ypeer % PLANE, zs * PLANE + xpeer % PLANE
        if n > 0:
            absorb(zs * PLANE + q)
        await_full(by)
        flying.append(ship(gath.at[by, upper], gath.at[by, upper], sent_dx.at[n], got_dx.at[by], "rows", xpeer))
        await_full(bx)
        flying.append(ship(gath.at[bx, lower], gath.at[bx, lower], sent_dy.at[n], got_dy.at[bx], "rows", ypeer))
        absorb(by)
        absorb(bx)
    for n, o in enumerate(delays):
        zs = (z + o) % planes
        bd = zs * PLANE + diag % PLANE
        await_part(bd, upper, got_dx)
        await_part(bd, lower, got_dy)
        absorb(bd)

    mine[1] = (pnorm + low[0:1, :]) / width
    min_copies.append(ship(mine.at[1], theirs.at[1], sent_min.at[1], got_min.at[1], "cent", partner))
    for copy in a2a + flying:
        copy.wait_send()
    for c in outs:
        c.wait()
    for n, copy in enumerate(min_copies):
        copy.wait()
        near_ref[n:n + 1, :] = jnp.minimum(mine[n], theirs[n])


def fused(points, centroids, assign, rows, cap, share):
    count_pts, width = points.shape
    planes = rows // PLANE
    pnorm = jnp.sum(jnp.square(points.astype(jnp.float32)), axis=1)[None, :]
    vmem = pl.BlockSpec(memory_space=pltpu.VMEM)
    dma = pltpu.SemaphoreType.DMA
    chunk = PLANE * cap
    near, upd = pl.pallas_call(
        functools.partial(lloyd_kernel, rows, cap, share),
        out_shape=(
            jax.ShapeDtypeStruct((2, count_pts), jnp.float32),
            jax.ShapeDtypeStruct((rows, share, width), jnp.bfloat16),
        ),
        in_specs=[vmem] * 4,
        out_specs=(vmem, pl.BlockSpec(memory_space=pl.ANY)),
        scratch_shapes=[
            pltpu.VMEM((planes, chunk, width), jnp.bfloat16),
            pltpu.VMEM((planes, chunk // LANES, 8, LANES), jnp.float32),
            pltpu.VMEM((rows, cap, width), jnp.bfloat16),
            pltpu.VMEM((rows, 8, LANES), jnp.float32),
            pltpu.VMEM((share, width), jnp.float32),
            pltpu.VMEM((rows, share, width), jnp.bfloat16),
            pltpu.VMEM((2, 1, count_pts), jnp.float32),
            pltpu.VMEM((2, 1, count_pts), jnp.float32),
            pltpu.VMEM((8, count_pts), jnp.float32),
            dma((rows,)), dma((rows,)), dma((rows,)), dma((rows,)), dma((2,)),
            dma((planes,)), dma((planes,)), dma((planes,)), dma((rows,)),
            dma((planes,)), dma((planes,)), dma((rows,)), dma((rows,)), dma((rows,)),
            dma((2,)), dma((2,)),
        ],
        compiler_params=pltpu.CompilerParams(
            collective_id=0, has_side_effects=True, vmem_limit_bytes=VMEM_BYTES
        ),
    )(assign[None, :], pnorm, points, centroids)
    return near, upd.reshape(rows * share, width)


def step(rows, cent, points, centroids, assign):
    count_pts = points.shape[0]
    blocksize = centroids.shape[0]
    share = blocksize // rows
    cap = max(2, 2 * count_pts // (rows * cent))
    power = share & (share - 1) == 0 and cap & (cap - 1) == 0
    fits = cent == 2 and rows % PLANE == 0 and share % 32 == 0 and 16 <= cap <= LANES
    even = count_pts % 256 == 0 and blocksize % 512 == 0 and (PLANE * cap) % LANES == 0
    if power and fits and even:
        return fused(points, centroids, assign, rows, cap, share)
    return per_device(points, centroids, assign)


def solution(mesh):
    return jax.shard_map(
        functools.partial(step, mesh.shape["rows"], mesh.shape["cent"]),
        mesh=mesh,
        in_specs=(P("rows", None), P("cent", None), P("rows")),
        out_specs=(P(None, "rows"), P("cent", None)),
        check_vma=False,
    )
```

```python
import functools

import jax
import jax.numpy as jnp
from jax import lax
from jax.experimental import pallas as pl
from jax.experimental.pallas import tpu as pltpu
from jax.sharding import PartitionSpec as P


def smallest(points, pnorm, cents):
    cnorm = jnp.sum(jnp.square(cents.astype(jnp.float32)), axis=1)
    dots = lax.dot_general(
        points, cents, (((1,), (1,)), ((), ())), preferred_element_type=jnp.float32
    )
    return jnp.min((pnorm[:, None] - 2.0 * dots + cnorm[None, :]) / points.shape[1], axis=1)


def block_min(values):
    return lax.pmin(values, "cent")


def renew(part_sums, part_counts, own_rows):
    return ((part_sums + own_rows.astype(jnp.float32)) / (part_counts[:, None] + 1.0)).astype(
        jnp.bfloat16
    )


def per_device(points, centroids, assign):
    blocksize = centroids.shape[0]
    count_pts = points.shape[0]
    pnorm = jnp.sum(jnp.square(points.astype(jnp.float32)), axis=1)
    first = smallest(points, pnorm, centroids)
    first = block_min(first)
    relative = assign - lax.axis_index("cent") * blocksize
    share = blocksize // lax.axis_size("rows")
    own = lax.dynamic_slice_in_dim(centroids, lax.axis_index("rows") * share, share, 0)
    rows_count = lax.axis_size("rows")
    groups = rows_count * lax.axis_size("cent")
    capacity = max(2, 2 * count_pts // groups)
    inside = (relative >= 0) & (relative < blocksize)
    owners = jnp.where(inside, relative // share, rows_count)
    offsets = jnp.where(inside, relative - relative // share * share, 0)
    owner_hot = owners[:, None] == lax.broadcasted_iota(jnp.int32, (count_pts, rows_count), 1)
    earlier = lax.broadcasted_iota(jnp.int32, (count_pts, count_pts), 1) < lax.broadcasted_iota(
        jnp.int32, (count_pts, count_pts), 0
    )
    before = jnp.dot(
        earlier.astype(jnp.bfloat16),
        owner_hot.astype(jnp.bfloat16),
        preferred_element_type=jnp.float32,
    )
    ranking = jnp.sum(jnp.where(owner_hot, before, 0.0), axis=1).astype(jnp.int32)
    slot_index = jnp.where(inside, owners * capacity + ranking, -1)
    placing = (
        lax.broadcasted_iota(jnp.int32, (rows_count * capacity, count_pts), 0)
        == slot_index[None, :]
    )
    outgoing = jnp.dot(
        placing.astype(jnp.bfloat16), points, preferred_element_type=jnp.float32
    ).astype(jnp.bfloat16)
    labels = (jnp.sum(jnp.where(placing, offsets[None, :] + 1, 0), axis=1) - 1).astype(jnp.bfloat16)
    arrived, arrived_labels = (
        lax.all_to_all(outgoing, "rows", split_axis=0, concat_axis=0, tiled=True),
        lax.all_to_all(labels, "rows", split_axis=0, concat_axis=0, tiled=True),
    )
    chosen = (
        lax.broadcasted_iota(jnp.int32, (share, arrived.shape[0]), 0)
        == arrived_labels.astype(jnp.int32)[None, :]
    )
    part_sums = jnp.dot(chosen.astype(jnp.bfloat16), arrived, preferred_element_type=jnp.float32)
    part_counts = jnp.sum(chosen.astype(jnp.float32), axis=1)
    updated = lax.all_gather(renew(part_sums, part_counts, own), "rows", axis=0, tiled=True)
    second = smallest(points, pnorm, updated)
    nearest = jnp.stack([first, block_min(second)])
    return (nearest, updated)


PLANE = 4
LANES = 128
VMEM_BYTES = 30 * 1024 * 1024


def nt_dot(a, b):
    return lax.dot_general(a, b, (((1,), (1,)), ((), ())), preferred_element_type=jnp.float32)


def column_min(cents, points):
    wide = cents.astype(jnp.float32)
    cnorm = jnp.sum(wide * wide, axis=1, keepdims=True)
    return jnp.min(cnorm - 2.0 * nt_dot(cents, points), axis=0, keepdims=True)


def lloyd_kernel(
    rows, cap, share, assign_ref, points_hbm, cents_hbm, near_ref, upd_ref,
    points_ref, cents_ref, load_sem,
    send, lab_send, arrived, lab_arrived, acc, gath, mine, theirs, low,
    sent_pts, got_pts, sent_lab, got_lab, own_sem,
    sent_up, sent_down, sent_x, sent_y, got_full, sent_dx, sent_dy, got_dx, got_dy, out_sem, sent_min, got_min,
):
    count_pts, width = points_ref.shape
    blocksize = cents_ref.shape[0]
    planes = rows // PLANE
    per = LANES // cap
    me = lax.axis_index("rows")
    core = lax.axis_index("cent")
    z, q = me // PLANE, me % PLANE
    xpeer = me + 1 - 2 * (q % 2)
    ypeer = me + 2 - 4 * (q // 2)
    diag = ypeer + 1 - 2 * (q % 2)
    partner = 1 - core

    points_in = pltpu.make_async_copy(points_hbm, points_ref, load_sem.at[0])
    points_in.start()
    cents_in = pltpu.make_async_copy(cents_hbm, cents_ref, load_sem.at[1])
    cents_in.start()
    barrier = pltpu.get_barrier_semaphore()
    for step in range(1, rows):
        pl.semaphore_signal(barrier, inc=1, device_id={"rows": (me + step) % rows})
    pl.semaphore_signal(barrier, inc=1, device_id={"cent": partner})

    relative = (assign_ref[...] - core * blocksize).astype(jnp.float32)
    inside = (relative >= 0.0) & (relative < float(blocksize))
    owner = jnp.where(inside, jnp.floor(relative * (1.0 / share)), float(rows))
    offset1 = jnp.where(inside, relative - owner * share + 1.0, 0.0)
    hot = lax.broadcasted_iota(jnp.int32, (rows, count_pts), 0).astype(jnp.float32) == owner
    hot_f = jnp.where(hot, 1.0, 0.0)
    seg = 256
    tri = jnp.where(
        lax.broadcasted_iota(jnp.int32, (seg, seg), 0) < lax.broadcasted_iota(jnp.int32, (seg, seg), 1),
        1.0, 0.0,
    ).astype(jnp.bfloat16)
    carry = jnp.zeros((rows, 1), jnp.float32)
    pieces = []
    for s in range(count_pts // seg):
        part = hot_f[:, s * seg:(s + 1) * seg]
        before = jnp.dot(part.astype(jnp.bfloat16), tri, preferred_element_type=jnp.float32) + carry
        pieces.append(jnp.sum(part * before, axis=0, keepdims=True))
        carry = carry + jnp.sum(part, axis=1, keepdims=True)
    ranking = jnp.concatenate(pieces, axis=1)
    slot = jnp.where(inside, owner * cap + ranking, -1.0)
    labels8 = jnp.broadcast_to(offset1, (8, count_pts)).astype(jnp.bfloat16)

    points_in.wait()
    pl.semaphore_wait(barrier, rows)

    order = [planes // 2] + [o for o in range(1, planes) if o != planes // 2] + [0]
    chunk = PLANE * cap
    a2a = []

    def ship(src, dst, ss, rs, axis, target):
        copy = pltpu.make_async_remote_copy(
            src_ref=src, dst_ref=dst, send_sem=ss, recv_sem=rs, device_id={axis: target}
        )
        copy.start()
        return copy

    own_copies = []
    for j, o in enumerate(order):
        zt = (z + o) % planes
        placing = jnp.where(
            (lax.broadcasted_iota(jnp.int32, (chunk, count_pts), 0) + zt * chunk).astype(jnp.float32)
            == slot, 1.0, 0.0,
        ).astype(jnp.bfloat16)
        lab = nt_dot(labels8, placing)
        for t in range(chunk // LANES):
            lab_send[j, t] = lab[:, t * LANES:(t + 1) * LANES]
        send[j] = jnp.dot(
            placing, points_ref[...], preferred_element_type=jnp.float32
        ).astype(jnp.bfloat16)
        for k in range(PLANE):
            i = (q + k) % PLANE
            target = zt * PLANE + i
            piece = send.at[j, pl.ds(pl.multiple_of(i * cap, cap), cap)]
            lab_piece = lab_send.at[j, i // per]
            spot = arrived.at[me]
            if o == 0 and k == 0:
                for n, (a, b) in enumerate(((piece, spot), (lab_piece, lab_arrived.at[me]))):
                    c = pltpu.make_async_copy(a, b, own_sem.at[n])
                    c.start()
                    own_copies.append(c)
            else:
                n = j * PLANE + k
                a2a.append(ship(lab_piece, lab_arrived.at[me], sent_lab.at[n], got_lab.at[me], "rows", target))
                a2a.append(ship(piece, spot, sent_pts.at[n], got_pts.at[me], "rows", target))

    squares = jnp.square(points_ref[...].astype(jnp.float32))
    high = squares.astype(jnp.bfloat16)
    rest = (squares - high.astype(jnp.float32)).astype(jnp.bfloat16)
    ones = jnp.ones((8, width), jnp.bfloat16)
    pnorm = (nt_dot(ones, high) + nt_dot(ones, rest))[0:1, :]
    cents_in.wait()
    kb = 512
    low[...] = jnp.full(low.shape, jnp.inf, jnp.float32)

    def first_step(i, _):
        block = cents_ref[pl.ds(pl.multiple_of(i * kb, kb), kb), :]
        low[0:1, :] = jnp.minimum(low[0:1, :], column_min(block, points_ref[...]))
        return 0

    lax.fori_loop(0, blocksize // kb, first_step, 0)
    mine[0] = (pnorm + low[0:1, :]) / width
    min_copies = [ship(mine.at[0], theirs.at[0], sent_min.at[0], got_min.at[0], "cent", partner)]

    acc[...] = jnp.zeros_like(acc)
    counts = jnp.zeros((share, 1), jnp.float32)
    rowid1 = lax.broadcasted_iota(jnp.int32, (share, cap), 0).astype(jnp.float32) + 1.0
    for c in own_copies:
        c.wait()
    for o in [0] + [o for o in order if o != 0]:
        zs = (z + planes - o) % planes
        total = None
        for k in range(PLANE):
            i = (q + PLANE - k) % PLANE
            source = zs * PLANE + i
            if not (o == 0 and k == 0):
                for ref, sem in ((lab_arrived, got_lab), (arrived, got_pts)):
                    pltpu.make_async_remote_copy(
                        src_ref=ref.at[source], dst_ref=ref.at[source], send_sem=own_sem.at[0],
                        recv_sem=sem.at[source], device_id={"rows": source},
                    ).wait_recv()
            lab = lab_arrived[source]
            pick = lab[0:1, 0:cap]
            for t in range(1, per):
                pick = jnp.where(q % per == t, lab[0:1, t * cap:(t + 1) * cap], pick)
            chosen = jnp.where(rowid1 == pick, 1.0, 0.0)
            counts = counts + jnp.sum(chosen, axis=1, keepdims=True)
            acc[...] += jnp.dot(
                chosen.astype(jnp.bfloat16), arrived[source], preferred_element_type=jnp.float32
            )
    own_rows = cents_ref[pl.ds(pl.multiple_of(me * share, share), share), :]
    gath[me] = ((acc[...] + own_rows.astype(jnp.float32)) / (counts + 1.0)).astype(jnp.bfloat16)

    flying = []
    outs = []
    half = share // 2

    def pass_on(block, n):
        flying.append(ship(gath.at[block], gath.at[block], sent_x.at[n], got_full.at[block], "rows", xpeer))
        flying.append(ship(gath.at[block], gath.at[block], sent_y.at[n], got_full.at[block], "rows", ypeer))

    def await_full(block):
        pltpu.make_async_remote_copy(
            src_ref=gath.at[block], dst_ref=gath.at[block], send_sem=own_sem.at[0],
            recv_sem=got_full.at[block], device_id={"rows": xpeer},
        ).wait_recv()

    def await_part(block, part, sem):
        pltpu.make_async_remote_copy(
            src_ref=gath.at[block, part], dst_ref=gath.at[block, part], send_sem=own_sem.at[0],
            recv_sem=sem.at[block], device_id={"rows": xpeer},
        ).wait_recv()

    low[...] = jnp.full(low.shape, jnp.inf, jnp.float32)

    def absorb(block):
        c = pltpu.make_async_copy(gath.at[block], upd_ref.at[block], out_sem.at[block])
        c.start()
        outs.append(c)
        low[0:1, :] = jnp.minimum(low[0:1, :], column_min(gath[block], points_ref[...]))

    climbs = []

    def climb(block, n, upward, downward):
        for allowed, sems, toward in ((upward, sent_up, PLANE), (downward, sent_down, -PLANE)):
            @pl.when(allowed)
            def _(sems=sems, toward=toward):
                ship(gath.at[block], gath.at[block], sems.at[n], got_full.at[block], "rows", me + toward)
            climbs.append((block, n, allowed, sems, toward))

    upper, lower = pl.ds(0, half), pl.ds(half, half)
    top = z // 2
    visits = [z, z + 1 - 2 * (z % 2), 2 - top, 3 - 3 * top]
    climb(me, 0, z < planes - 1, z > 0)
    pass_on(me, 0)
    absorb(me)

    def cross(n):
        by, bx = visits[n] * PLANE + ypeer % PLANE, visits[n] * PLANE + xpeer % PLANE
        await_full(by)
        flying.append(ship(gath.at[by, upper], gath.at[by, upper], sent_dx.at[n], got_dx.at[by], "rows", xpeer))
        await_full(bx)
        flying.append(ship(gath.at[bx, lower], gath.at[bx, lower], sent_dy.at[n], got_dy.at[bx], "rows", ypeer))
        return by, bx

    for n in range(1, planes):
        zs = visits[n]
        block = zs * PLANE + q
        await_full(block)
        climb(block, n, (zs < z) & (z < planes - 1), (zs > z) & (z > 0))
        pass_on(block, n)
        ready = cross(n - 1)
        absorb(block)
        for b in ready:
            absorb(b)
    for b in cross(planes - 1):
        absorb(b)
    for zs in visits:
        bd = zs * PLANE + diag % PLANE
        await_part(bd, upper, got_dx)
        await_part(bd, lower, got_dy)
        absorb(bd)

    mine[1] = (pnorm + low[0:1, :]) / width
    min_copies.append(ship(mine.at[1], theirs.at[1], sent_min.at[1], got_min.at[1], "cent", partner))
    for copy in a2a + flying:
        copy.wait_send()
    for block, n, allowed, sems, toward in climbs:
        @pl.when(allowed)
        def _(block=block, n=n, sems=sems, toward=toward):
            pltpu.make_async_remote_copy(
                src_ref=gath.at[block], dst_ref=gath.at[block], send_sem=sems.at[n],
                recv_sem=got_full.at[block], device_id={"rows": me + toward},
            ).wait_send()
    for c in outs:
        c.wait()
    for n, copy in enumerate(min_copies):
        copy.wait()
        near_ref[n:n + 1, :] = jnp.minimum(mine[n], theirs[n])


def fused(points, centroids, assign, rows, cap, share):
    count_pts, width = points.shape
    planes = rows // PLANE
    hbm = pl.BlockSpec(memory_space=pltpu.HBM)
    vmem = pl.BlockSpec(memory_space=pltpu.VMEM)
    dma = pltpu.SemaphoreType.DMA
    chunk = PLANE * cap
    near, upd = pl.pallas_call(
        functools.partial(lloyd_kernel, rows, cap, share),
        out_shape=(
            jax.ShapeDtypeStruct((2, count_pts), jnp.float32),
            jax.ShapeDtypeStruct((rows, share, width), jnp.bfloat16),
        ),
        in_specs=[vmem, hbm, hbm],
        out_specs=(vmem, pl.BlockSpec(memory_space=pl.ANY)),
        scratch_shapes=[
            pltpu.VMEM((count_pts, width), jnp.bfloat16),
            pltpu.VMEM(centroids.shape, jnp.bfloat16),
            dma((2,)),
            pltpu.VMEM((planes, chunk, width), jnp.bfloat16),
            pltpu.VMEM((planes, chunk // LANES, 8, LANES), jnp.float32),
            pltpu.VMEM((rows, cap, width), jnp.bfloat16),
            pltpu.VMEM((rows, 8, LANES), jnp.float32),
            pltpu.VMEM((share, width), jnp.float32),
            pltpu.VMEM((rows, share, width), jnp.bfloat16),
            pltpu.VMEM((2, 1, count_pts), jnp.float32),
            pltpu.VMEM((2, 1, count_pts), jnp.float32),
            pltpu.VMEM((8, count_pts), jnp.float32),
            dma((rows,)), dma((rows,)), dma((rows,)), dma((rows,)), dma((2,)),
            dma((planes,)), dma((planes,)), dma((planes,)), dma((planes,)), dma((rows,)),
            dma((planes,)), dma((planes,)), dma((rows,)), dma((rows,)), dma((rows,)),
            dma((2,)), dma((2,)),
        ],
        compiler_params=pltpu.CompilerParams(
            collective_id=0, has_side_effects=True, vmem_limit_bytes=VMEM_BYTES
        ),
    )(assign[None, :], points, centroids)
    return near, upd.reshape(rows * share, width)


def step(rows, cent, points, centroids, assign):
    count_pts = points.shape[0]
    blocksize = centroids.shape[0]
    share = blocksize // rows
    cap = max(2, 2 * count_pts // (rows * cent))
    power = share & (share - 1) == 0 and cap & (cap - 1) == 0
    fits = cent == 2 and rows == 4 * PLANE and share % 32 == 0 and 16 <= cap <= LANES
    even = count_pts % 256 == 0 and blocksize % 512 == 0 and (PLANE * cap) % LANES == 0
    if power and fits and even:
        return fused(points, centroids, assign, rows, cap, share)
    return per_device(points, centroids, assign)


def solution(mesh):
    return jax.shard_map(
        functools.partial(step, mesh.shape["rows"], mesh.shape["cent"]),
        mesh=mesh,
        in_specs=(P("rows", None), P("cent", None), P("rows")),
        out_specs=(P(None, "rows"), P("cent", None)),
        check_vma=False,
    )
```

```python
import functools

import jax
import jax.numpy as jnp
from jax import lax
from jax.experimental import pallas as pl
from jax.experimental.pallas import tpu as pltpu
from jax.sharding import PartitionSpec as P


def smallest(points, pnorm, cents):
    cnorm = jnp.sum(jnp.square(cents.astype(jnp.float32)), axis=1)
    dots = lax.dot_general(
        points, cents, (((1,), (1,)), ((), ())), preferred_element_type=jnp.float32
    )
    return jnp.min((pnorm[:, None] - 2.0 * dots + cnorm[None, :]) / points.shape[1], axis=1)


def block_min(values):
    return lax.pmin(values, "cent")


def renew(part_sums, part_counts, own_rows):
    return ((part_sums + own_rows.astype(jnp.float32)) / (part_counts[:, None] + 1.0)).astype(
        jnp.bfloat16
    )


def per_device(points, centroids, assign):
    blocksize = centroids.shape[0]
    count_pts = points.shape[0]
    pnorm = jnp.sum(jnp.square(points.astype(jnp.float32)), axis=1)
    first = smallest(points, pnorm, centroids)
    first = block_min(first)
    relative = assign - lax.axis_index("cent") * blocksize
    share = blocksize // lax.axis_size("rows")
    own = lax.dynamic_slice_in_dim(centroids, lax.axis_index("rows") * share, share, 0)
    rows_count = lax.axis_size("rows")
    groups = rows_count * lax.axis_size("cent")
    capacity = max(2, 2 * count_pts // groups)
    inside = (relative >= 0) & (relative < blocksize)
    owners = jnp.where(inside, relative // share, rows_count)
    offsets = jnp.where(inside, relative - relative // share * share, 0)
    owner_hot = owners[:, None] == lax.broadcasted_iota(jnp.int32, (count_pts, rows_count), 1)
    earlier = lax.broadcasted_iota(jnp.int32, (count_pts, count_pts), 1) < lax.broadcasted_iota(
        jnp.int32, (count_pts, count_pts), 0
    )
    before = jnp.dot(
        earlier.astype(jnp.bfloat16),
        owner_hot.astype(jnp.bfloat16),
        preferred_element_type=jnp.float32,
    )
    ranking = jnp.sum(jnp.where(owner_hot, before, 0.0), axis=1).astype(jnp.int32)
    slot_index = jnp.where(inside, owners * capacity + ranking, -1)
    placing = (
        lax.broadcasted_iota(jnp.int32, (rows_count * capacity, count_pts), 0)
        == slot_index[None, :]
    )
    outgoing = jnp.dot(
        placing.astype(jnp.bfloat16), points, preferred_element_type=jnp.float32
    ).astype(jnp.bfloat16)
    labels = (jnp.sum(jnp.where(placing, offsets[None, :] + 1, 0), axis=1) - 1).astype(jnp.bfloat16)
    arrived, arrived_labels = (
        lax.all_to_all(outgoing, "rows", split_axis=0, concat_axis=0, tiled=True),
        lax.all_to_all(labels, "rows", split_axis=0, concat_axis=0, tiled=True),
    )
    chosen = (
        lax.broadcasted_iota(jnp.int32, (share, arrived.shape[0]), 0)
        == arrived_labels.astype(jnp.int32)[None, :]
    )
    part_sums = jnp.dot(chosen.astype(jnp.bfloat16), arrived, preferred_element_type=jnp.float32)
    part_counts = jnp.sum(chosen.astype(jnp.float32), axis=1)
    updated = lax.all_gather(renew(part_sums, part_counts, own), "rows", axis=0, tiled=True)
    second = smallest(points, pnorm, updated)
    nearest = jnp.stack([first, block_min(second)])
    return (nearest, updated)


PLANE = 4
LANES = 128
VMEM_BYTES = 53 * 1024 * 1024


def nt_dot(a, b):
    return lax.dot_general(a, b, (((1,), (1,)), ((), ())), preferred_element_type=jnp.float32)


def column_min(cents, points):
    wide = cents.astype(jnp.float32)
    cnorm = jnp.sum(wide * wide, axis=1, keepdims=True)
    return jnp.min(cnorm - 2.0 * nt_dot(cents, points), axis=0, keepdims=True)


def lloyd_kernel(
    rows, cap, share, assign_ref, points_hbm, cents_hbm, near_ref, upd_ref,
    points_ref, cents_ref, load_sem,
    send, lab_send, arrived, lab_arrived, acc, gath, mine, theirs, low,
    sent_pts, got_pts, sent_lab, got_lab, own_sem,
    sent_up, sent_down, sent_x, sent_y, got_full, sent_dx, sent_dy, got_dx, got_dy, out_sem, sent_min, got_min,
):
    count_pts, width = points_ref.shape
    blocksize = cents_ref.shape[0]
    planes = rows // PLANE
    per = LANES // cap
    me = lax.axis_index("rows")
    core = lax.axis_index("cent")
    z, q = me // PLANE, me % PLANE
    xpeer = me + 1 - 2 * (q % 2)
    ypeer = me + 2 - 4 * (q // 2)
    diag = ypeer + 1 - 2 * (q % 2)
    partner = 1 - core

    points_in = pltpu.make_async_copy(points_hbm, points_ref, load_sem.at[0])
    points_in.start()
    cents_in = pltpu.make_async_copy(cents_hbm, cents_ref, load_sem.at[1])
    cents_in.start()
    barrier = pltpu.get_barrier_semaphore()
    for step in range(1, rows):
        pl.semaphore_signal(barrier, inc=1, device_id={"rows": (me + step) % rows})
    pl.semaphore_signal(barrier, inc=1, device_id={"cent": partner})

    relative = (assign_ref[...] - core * blocksize).astype(jnp.float32)
    inside = (relative >= 0.0) & (relative < float(blocksize))
    owner = jnp.where(inside, jnp.floor(relative * (1.0 / share)), float(rows))
    offset1 = jnp.where(inside, relative - owner * share + 1.0, 0.0)
    hot = lax.broadcasted_iota(jnp.int32, (rows, count_pts), 0).astype(jnp.float32) == owner
    hot_f = jnp.where(hot, 1.0, 0.0)
    seg = 256
    tri = jnp.where(
        lax.broadcasted_iota(jnp.int32, (seg, seg), 0) < lax.broadcasted_iota(jnp.int32, (seg, seg), 1),
        1.0, 0.0,
    ).astype(jnp.bfloat16)
    carry = jnp.zeros((rows, 1), jnp.float32)
    pieces = []
    for s in range(count_pts // seg):
        part = hot_f[:, s * seg:(s + 1) * seg]
        before = jnp.dot(part.astype(jnp.bfloat16), tri, preferred_element_type=jnp.float32) + carry
        pieces.append(jnp.sum(part * before, axis=0, keepdims=True))
        carry = carry + jnp.sum(part, axis=1, keepdims=True)
    ranking = jnp.concatenate(pieces, axis=1)
    slot = jnp.where(inside, owner * cap + ranking, -1.0)
    labels8 = jnp.broadcast_to(offset1, (8, count_pts)).astype(jnp.bfloat16)

    points_in.wait()
    pl.semaphore_wait(barrier, rows)

    order = [planes // 2] + [o for o in range(1, planes) if o != planes // 2] + [0]
    chunk = PLANE * cap
    a2a = []

    def ship(src, dst, ss, rs, axis, target):
        copy = pltpu.make_async_remote_copy(
            src_ref=src, dst_ref=dst, send_sem=ss, recv_sem=rs, device_id={axis: target}
        )
        copy.start()
        return copy

    own_copies = []
    for j, o in enumerate(order):
        zt = (z + o) % planes
        placing = jnp.where(
            (lax.broadcasted_iota(jnp.int32, (chunk, count_pts), 0) + zt * chunk).astype(jnp.float32)
            == slot, 1.0, 0.0,
        ).astype(jnp.bfloat16)
        lab = nt_dot(labels8, placing)
        for t in range(chunk // LANES):
            lab_send[j, t] = lab[:, t * LANES:(t + 1) * LANES]
        send[j] = jnp.dot(
            placing, points_ref[...], preferred_element_type=jnp.float32
        ).astype(jnp.bfloat16)
        for k in range(PLANE):
            i = (q + k) % PLANE
            target = zt * PLANE + i
            piece = send.at[j, pl.ds(pl.multiple_of(i * cap, cap), cap)]
            lab_piece = lab_send.at[j, i // per]
            spot = arrived.at[me]
            if o == 0 and k == 0:
                for n, (a, b) in enumerate(((piece, spot), (lab_piece, lab_arrived.at[me]))):
                    c = pltpu.make_async_copy(a, b, own_sem.at[n])
                    c.start()
                    own_copies.append(c)
            else:
                n = j * PLANE + k
                a2a.append(ship(lab_piece, lab_arrived.at[me], sent_lab.at[n], got_lab.at[me], "rows", target))
                a2a.append(ship(piece, spot, sent_pts.at[n], got_pts.at[me], "rows", target))

    squares = jnp.square(points_ref[...].astype(jnp.float32))
    high = squares.astype(jnp.bfloat16)
    rest = (squares - high.astype(jnp.float32)).astype(jnp.bfloat16)
    ones = jnp.ones((8, width), jnp.bfloat16)
    pnorm = (nt_dot(ones, high) + nt_dot(ones, rest))[0:1, :]
    cents_in.wait()
    kb = 512
    low[...] = jnp.full(low.shape, jnp.inf, jnp.float32)

    def first_step(i, _):
        block = cents_ref[pl.ds(pl.multiple_of(i * kb, kb), kb), :]
        low[0:1, :] = jnp.minimum(low[0:1, :], column_min(block, points_ref[...]))
        return 0

    lax.fori_loop(0, blocksize // kb, first_step, 0)
    mine[0] = (pnorm + low[0:1, :]) / width
    min_copies = [ship(mine.at[0], theirs.at[0], sent_min.at[0], got_min.at[0], "cent", partner)]

    acc[...] = jnp.zeros_like(acc)
    counts = jnp.zeros((share, 1), jnp.float32)
    rowid1 = lax.broadcasted_iota(jnp.int32, (share, cap), 0).astype(jnp.float32) + 1.0
    for c in own_copies:
        c.wait()
    for o in [0] + [o for o in order if o != 0]:
        zs = (z + planes - o) % planes
        total = None
        for k in range(PLANE):
            i = (q + PLANE - k) % PLANE
            source = zs * PLANE + i
            if not (o == 0 and k == 0):
                for ref, sem in ((lab_arrived, got_lab), (arrived, got_pts)):
                    pltpu.make_async_remote_copy(
                        src_ref=ref.at[source], dst_ref=ref.at[source], send_sem=own_sem.at[0],
                        recv_sem=sem.at[source], device_id={"rows": source},
                    ).wait_recv()
            lab = lab_arrived[source]
            pick = lab[0:1, 0:cap]
            for t in range(1, per):
                pick = jnp.where(q % per == t, lab[0:1, t * cap:(t + 1) * cap], pick)
            chosen = jnp.where(rowid1 == pick, 1.0, 0.0)
            counts = counts + jnp.sum(chosen, axis=1, keepdims=True)
            acc[...] += jnp.dot(
                chosen.astype(jnp.bfloat16), arrived[source], preferred_element_type=jnp.float32
            )
    own_rows = cents_ref[pl.ds(pl.multiple_of(me * share, share), share), :]
    gath[me] = ((acc[...] + own_rows.astype(jnp.float32)) / (counts + 1.0)).astype(jnp.bfloat16)

    flying = []
    outs = []
    half = share // 2

    def pass_on(block, n):
        flying.append(ship(gath.at[block], gath.at[block], sent_x.at[n], got_full.at[block], "rows", xpeer))
        flying.append(ship(gath.at[block], gath.at[block], sent_y.at[n], got_full.at[block], "rows", ypeer))

    def await_full(block):
        pltpu.make_async_remote_copy(
            src_ref=gath.at[block], dst_ref=gath.at[block], send_sem=own_sem.at[0],
            recv_sem=got_full.at[block], device_id={"rows": xpeer},
        ).wait_recv()

    def await_part(block, part, sem):
        pltpu.make_async_remote_copy(
            src_ref=gath.at[block, part], dst_ref=gath.at[block, part], send_sem=own_sem.at[0],
            recv_sem=sem.at[block], device_id={"rows": xpeer},
        ).wait_recv()

    low[...] = jnp.full(low.shape, jnp.inf, jnp.float32)

    def absorb(block):
        c = pltpu.make_async_copy(gath.at[block], upd_ref.at[block], out_sem.at[block])
        c.start()
        outs.append(c)
        low[0:1, :] = jnp.minimum(low[0:1, :], column_min(gath[block], points_ref[...]))

    climbs = []

    def climb(block, n, upward, downward):
        for allowed, sems, toward in ((upward, sent_up, PLANE), (downward, sent_down, -PLANE)):
            @pl.when(allowed)
            def _(sems=sems, toward=toward):
                ship(gath.at[block], gath.at[block], sems.at[n], got_full.at[block], "rows", me + toward)
            climbs.append((block, n, allowed, sems, toward))

    upper, lower = pl.ds(0, half), pl.ds(half, half)
    top = z // 2
    visits = [z, z + 1 - 2 * (z % 2), 2 - top, 3 - 3 * top]
    climb(me, 0, z < planes - 1, z > 0)
    pass_on(me, 0)
    absorb(me)

    def cross(n):
        by, bx = visits[n] * PLANE + ypeer % PLANE, visits[n] * PLANE + xpeer % PLANE
        await_full(by)
        flying.append(ship(gath.at[by, upper], gath.at[by, upper], sent_dx.at[n], got_dx.at[by], "rows", xpeer))
        await_full(bx)
        flying.append(ship(gath.at[bx, lower], gath.at[bx, lower], sent_dy.at[n], got_dy.at[bx], "rows", ypeer))
        return by, bx

    for n in range(1, planes):
        zs = visits[n]
        block = zs * PLANE + q
        await_full(block)
        climb(block, n, (zs < z) & (z < planes - 1), (zs > z) & (z > 0))
        pass_on(block, n)
        ready = cross(n - 1)
        absorb(block)
        for b in ready:
            absorb(b)
    for b in cross(planes - 1):
        absorb(b)
    for zs in visits:
        bd = zs * PLANE + diag % PLANE
        await_part(bd, upper, got_dx)
        await_part(bd, lower, got_dy)
        absorb(bd)

    mine[1] = (pnorm + low[0:1, :]) / width
    min_copies.append(ship(mine.at[1], theirs.at[1], sent_min.at[1], got_min.at[1], "cent", partner))
    for copy in a2a + flying:
        copy.wait_send()
    for block, n, allowed, sems, toward in climbs:
        @pl.when(allowed)
        def _(block=block, n=n, sems=sems, toward=toward):
            pltpu.make_async_remote_copy(
                src_ref=gath.at[block], dst_ref=gath.at[block], send_sem=sems.at[n],
                recv_sem=got_full.at[block], device_id={"rows": me + toward},
            ).wait_send()
    for c in outs:
        c.wait()
    for n, copy in enumerate(min_copies):
        copy.wait()
        near_ref[n:n + 1, :] = jnp.minimum(mine[n], theirs[n])


def fused(points, centroids, assign, rows, cap, share):
    count_pts, width = points.shape
    planes = rows // PLANE
    hbm = pl.BlockSpec(memory_space=pltpu.HBM)
    vmem = pl.BlockSpec(memory_space=pltpu.VMEM)
    dma = pltpu.SemaphoreType.DMA
    chunk = PLANE * cap
    near, upd = pl.pallas_call(
        functools.partial(lloyd_kernel, rows, cap, share),
        out_shape=(
            jax.ShapeDtypeStruct((2, count_pts), jnp.float32),
            jax.ShapeDtypeStruct((rows, share, width), jnp.bfloat16),
        ),
        in_specs=[vmem, hbm, hbm],
        out_specs=(vmem, pl.BlockSpec(memory_space=pl.ANY)),
        scratch_shapes=[
            pltpu.VMEM((count_pts, width), jnp.bfloat16),
            pltpu.VMEM(centroids.shape, jnp.bfloat16),
            dma((2,)),
            pltpu.VMEM((planes, chunk, width), jnp.bfloat16),
            pltpu.VMEM((planes, chunk // LANES, 8, LANES), jnp.float32),
            pltpu.VMEM((rows, cap, width), jnp.bfloat16),
            pltpu.VMEM((rows, 8, LANES), jnp.float32),
            pltpu.VMEM((share, width), jnp.float32),
            pltpu.VMEM((rows, share, width), jnp.bfloat16),
            pltpu.VMEM((2, 1, count_pts), jnp.float32),
            pltpu.VMEM((2, 1, count_pts), jnp.float32),
            pltpu.VMEM((8, count_pts), jnp.float32),
            dma((rows,)), dma((rows,)), dma((rows,)), dma((rows,)), dma((2,)),
            dma((planes,)), dma((planes,)), dma((planes,)), dma((planes,)), dma((rows,)),
            dma((planes,)), dma((planes,)), dma((rows,)), dma((rows,)), dma((rows,)),
            dma((2,)), dma((2,)),
        ],
        compiler_params=pltpu.CompilerParams(
            collective_id=0, has_side_effects=True, vmem_limit_bytes=VMEM_BYTES
        ),
    )(assign[None, :], points, centroids)
    return near, upd.reshape(rows * share, width)


def step(rows, cent, points, centroids, assign):
    count_pts = points.shape[0]
    blocksize = centroids.shape[0]
    share = blocksize // rows
    cap = max(2, 2 * count_pts // (rows * cent))
    power = share & (share - 1) == 0 and cap & (cap - 1) == 0
    fits = cent == 2 and rows == 4 * PLANE and share % 32 == 0 and 16 <= cap <= LANES
    even = count_pts % 256 == 0 and blocksize % 512 == 0 and (PLANE * cap) % LANES == 0
    if power and fits and even:
        return fused(points, centroids, assign, rows, cap, share)
    return per_device(points, centroids, assign)


def solution(mesh):
    return jax.shard_map(
        functools.partial(step, mesh.shape["rows"], mesh.shape["cent"]),
        mesh=mesh,
        in_specs=(P("rows", None), P("cent", None), P("rows")),
        out_specs=(P(None, "rows"), P("cent", None)),
        check_vma=False,
    )
```
